32 devices in a mesh: cond: 2 (over core), kern: 2 (over y), tile: 8 (over z, x).
Axes of the slice: x: 2, y: 2, z: 4, core: 2. Of those that a mesh axis runs over, the one named last changes fastest.
Arguments:
- mask: bfloat16 [1, 1024, 1024], P(None, 'tile'), may hold values from -6 to 6
- kernels: bfloat16 [2, 4, 24, 512, 512], P(None, 'cond', 'kern', 'tile'), may hold values from -6 to 6
- kernel_weights: float32 [4, 24], P('cond', 'kern'), may hold values from 0.02 to 0.2
Outputs:
- low: float32 [1, 1024, 1024], P(None, 'tile', 'kern')
- high: float32 [1, 1024, 1024], P(None, 'tile', 'kern')
The draws below stay inside these ranges and needn't reach their ends.
All inputs are finite; a program needn't handle non-finite values.
Results may differ from the reference program's by a relative error of at most 0.0032.
Values may be sent and summed in bfloat16 or wider, within the bound.
A program may use at most 128 MiB of HBM per device.

```python
import math
import jax
import jax.numpy as jnp
from jax import lax

P_SIZE = 1024
B = 512
KERNELS = 24
CONDS = 4
TILES = 1


def steps_of(own_key, shape, split, smallest, largest):
    factor_of = 1.0
    for dim, parts in split:
        steps = jax.random.uniform(jax.random.fold_in(jax.random.fold_in(own_key, 6), dim), (parts,), jnp.float32, smallest / len(split), largest / len(split))
        factor_of = factor_of * jnp.repeat(jnp.exp(steps), shape[dim] // parts).reshape((-1,) + (1,) * (len(shape) - 1 - dim))
    return factor_of


def normal_values(own_key, dims, scale, most, split=(), held_as=jnp.bfloat16):
    values = scale * jax.random.normal(own_key, dims, jnp.float32)
    if split:
        values = values * steps_of(own_key, dims, split, -0.22, 0.18)
    return jnp.clip(values, -most, most).astype(held_as)


def setup_inputs(seed: int = 0) -> dict:
    keys = jax.random.split(jax.random.key(seed), 4)
    return {
        "mask": normal_values(keys[0], (TILES, P_SIZE, P_SIZE), 1.0, 6.0, ((1, 8),)),
        "kernels": normal_values(keys[1], (2, CONDS, KERNELS, B, B), 1.0, 6.0, ((1, 2), (2, 2), (3, 8))),
        "kernel_weights": jnp.clip(jnp.exp(math.log(0.2) - 2.3025851 * jax.random.uniform(keys[2], (CONDS, KERNELS), jnp.float32) ** steps_of(keys[2], (CONDS, KERNELS), ((0, 2), (1, 2)), -0.2, 0.2)), 0.02, 0.2),
    }


def tables(length, count):
    pixel = jnp.arange(length, dtype=jnp.int32)[:, None]
    freq = jnp.arange(count, dtype=jnp.int32)[None, :] - count // 2
    phase = jnp.mod(pixel * freq, length).astype(jnp.float32) * (2.0 * math.pi / length)
    factor = 1.0 / math.sqrt(length)
    return ((jnp.cos(phase) * factor).astype(jnp.bfloat16), (jnp.sin(phase) * factor).astype(jnp.bfloat16))

def product(left, right):
    return jnp.dot(left, right, preferred_element_type=jnp.float32)

def reference(mask, kernels, kernel_weights):
    cos_table, sin_table = tables(P_SIZE, B)
    cos_back = cos_table.T
    sin_back = sin_table.T

    def one_tile(tile):
        row_re = product(tile, cos_table).astype(jnp.bfloat16)
        row_im = (-product(tile, sin_table)).astype(jnp.bfloat16)
        spec_re = product(row_re.T, cos_table) + product(row_im.T, sin_table)
        spec_im = product(row_im.T, cos_table) - product(row_re.T, sin_table)

        def one_cond(inputs):
            cond_re, cond_im, weights = inputs

            def add_kernel(total, item):
                kern_re, kern_im, weight = item
                kern_re = kern_re.astype(jnp.float32)
                kern_im = kern_im.astype(jnp.float32)
                filt_re = (spec_re * kern_re - spec_im * kern_im).astype(jnp.bfloat16)
                filt_im = (spec_re * kern_im + spec_im * kern_re).astype(jnp.bfloat16)
                half_re = (product(filt_re, cos_back) - product(filt_im, sin_back)).astype(jnp.bfloat16)
                half_im = (product(filt_re, sin_back) + product(filt_im, cos_back)).astype(jnp.bfloat16)
                field_re = product(half_re.T, cos_back) - product(half_im.T, sin_back)
                field_im = product(half_re.T, sin_back) + product(half_im.T, cos_back)
                return (total + weight * (field_re * field_re + field_im * field_im), None)
            start = jnp.zeros((P_SIZE, P_SIZE), jnp.float32)
            total, _ = lax.scan(add_kernel, start, (cond_re, cond_im, weights))
            return total
        intensity = lax.map(one_cond, (kernels[0], kernels[1], kernel_weights))
        return (lax.optimization_barrier(jnp.min(intensity, axis=0)), lax.optimization_barrier(jnp.max(intensity, axis=0)))
    low, high = lax.map(one_tile, mask)
    return (low, high)
```

```python
import functools
import math

import jax
import jax.numpy as jnp
import numpy as np
from jax import lax
from jax.experimental import pallas as pl
from jax.experimental.pallas import tpu as pltpu
from jax.sharding import PartitionSpec as P


def tables(length, count):
    pixel = jnp.arange(length, dtype=jnp.int32)[:, None]
    freq = jnp.arange(count, dtype=jnp.int32)[None, :] - count // 2
    phase = jnp.mod(pixel * freq, length).astype(jnp.float32) * (2.0 * math.pi / length)
    factor = 1.0 / math.sqrt(length)
    return (
        (jnp.cos(phase) * factor).astype(jnp.bfloat16),
        (jnp.sin(phase) * factor).astype(jnp.bfloat16),
    )


def field_power(half_re, half_im, cos_table, sin_table):
    field_re = jnp.einsum("tnjr,pj->tnrp", half_re, cos_table, preferred_element_type=jnp.float32)
    field_re = field_re - jnp.einsum(
        "tnjr,pj->tnrp", half_im, sin_table, preferred_element_type=jnp.float32
    )
    field_im = jnp.einsum("tnjr,pj->tnrp", half_re, sin_table, preferred_element_type=jnp.float32)
    field_im = field_im + jnp.einsum(
        "tnjr,pj->tnrp", half_im, cos_table, preferred_element_type=jnp.float32
    )
    return field_re * field_re + field_im * field_im


def filter_spectrum(spec_re, spec_im, kern_re, kern_im):
    kern_re = kern_re.astype(jnp.float32)
    kern_im = kern_im.astype(jnp.float32)
    filt_re = spec_re[:, None] * kern_re[None] - spec_im[:, None] * kern_im[None]
    filt_im = spec_re[:, None] * kern_im[None] + spec_im[:, None] * kern_re[None]
    return (filt_re.astype(jnp.bfloat16), filt_im.astype(jnp.bfloat16))


def half_transform(filt_re, filt_im, cos_part, sin_part):
    half_re = jnp.einsum("tnji,ri->tnjr", filt_re, cos_part, preferred_element_type=jnp.float32)
    half_re = half_re - jnp.einsum(
        "tnji,ri->tnjr", filt_im, sin_part, preferred_element_type=jnp.float32
    )
    half_im = jnp.einsum("tnji,ri->tnjr", filt_re, sin_part, preferred_element_type=jnp.float32)
    half_im = half_im + jnp.einsum(
        "tnji,ri->tnjr", filt_im, cos_part, preferred_element_type=jnp.float32
    )
    return (half_re.astype(jnp.bfloat16), half_im.astype(jnp.bfloat16))


def column_spectrum(rows_re, rows_im, cos_part, sin_part):
    spec_re = jnp.einsum("tjr,ri->tji", rows_re, cos_part, preferred_element_type=jnp.float32)
    spec_re = spec_re + jnp.einsum(
        "tjr,ri->tji", rows_im, sin_part, preferred_element_type=jnp.float32
    )
    spec_im = jnp.einsum("tjr,ri->tji", rows_im, cos_part, preferred_element_type=jnp.float32)
    spec_im = spec_im - jnp.einsum(
        "tjr,ri->tji", rows_re, sin_part, preferred_element_type=jnp.float32
    )
    return (spec_re, spec_im)


def local(mask, kernels, kernel_weights):
    tiles_here, rows, pixels = mask.shape
    count = kernels.shape[4]
    conds, kerns = kernel_weights.shape
    items = conds * kerns
    cos_table, sin_table = tables(pixels, count)
    row_re = jnp.einsum("trc,cj->tjr", mask, cos_table, preferred_element_type=jnp.float32).astype(
        jnp.bfloat16
    )
    row_im = (
        -jnp.einsum("trc,cj->tjr", mask, sin_table, preferred_element_type=jnp.float32)
    ).astype(jnp.bfloat16)
    cols_re, cols_im = (
        lax.all_to_all(row_re, "tile", split_axis=1, concat_axis=2, tiled=True),
        lax.all_to_all(row_im, "tile", split_axis=1, concat_axis=2, tiled=True),
    )
    spec_re, spec_im = column_spectrum(cols_re, cols_im, cos_table, sin_table)
    freq_here = kernels.shape[3]
    kern_re = kernels[0].reshape(items, freq_here, count)
    kern_im = kernels[1].reshape(items, freq_here, count)
    filt_re, filt_im = filter_spectrum(spec_re, spec_im, kern_re, kern_im)
    half_re, half_im = half_transform(filt_re, filt_im, cos_table, sin_table)
    power = field_power(
        lax.all_to_all(half_re, "tile", split_axis=3, concat_axis=2, tiled=True),
        lax.all_to_all(half_im, "tile", split_axis=3, concat_axis=2, tiled=True),
        cos_table,
        sin_table,
    )
    power = power.reshape(tiles_here, conds, kerns, rows, pixels)
    weighted = jnp.einsum("tckrp,ck->tcrp", power, kernel_weights, precision=lax.Precision.HIGHEST)
    intensity = lax.psum_scatter(weighted, "kern", scatter_dimension=3, tiled=True)
    local_low = jnp.min(intensity, axis=1)
    local_high = jnp.max(intensity, axis=1)
    low = lax.pmin(local_low, "cond")
    high = lax.pmax(local_high, "cond")
    return (low, high)


def host_tables(length, count):
    pixel = np.arange(length, dtype=np.int64)[:, None]
    freq = np.arange(count, dtype=np.int64)[None, :] - count // 2
    phase = np.mod(pixel * freq, length).astype(np.float64) * (2.0 * math.pi / length)
    factor = 1.0 / math.sqrt(length)
    return np.cos(phase) * factor, np.sin(phase) * factor


def filter_kernel(core_ref, spec_ref, kept_ref, came_ref, out_ref):
    freqs, count = spec_ref.shape[1:]
    half = freqs // 2
    row = lax.broadcasted_iota(jnp.int32, (freqs, freqs), 0)
    col = lax.broadcasted_iota(jnp.int32, (freqs, freqs), 1)
    source = jnp.where(row < half, 2 * row, 2 * (row - half) + 1)
    order = (col == source).astype(jnp.bfloat16)
    spec_re = spec_ref[0]
    spec_im = spec_ref[1]

    def apply(kern_ref):
        chunks = kern_ref.shape[2]
        for part in range(kern_ref.shape[1] * chunks):
            kern_re = kern_ref[0, part // chunks, part % chunks].astype(jnp.float32)
            kern_im = kern_ref[1, part // chunks, part % chunks].astype(jnp.float32)
            filt_re = (spec_re * kern_re - spec_im * kern_im).astype(jnp.bfloat16)
            filt_im = (spec_re * kern_im + spec_im * kern_re).astype(jnp.bfloat16)
            out_ref[part, 0] = jnp.dot(order, filt_re, preferred_element_type=jnp.float32).astype(
                jnp.bfloat16
            )
            out_ref[part, 1] = jnp.dot(order, filt_im, preferred_element_type=jnp.float32).astype(
                jnp.bfloat16
            )

    mine = pl.program_id(0) == core_ref[0]

    @pl.when(mine)
    def _():
        apply(kept_ref)

    @pl.when(jnp.logical_not(mine))
    def _():
        apply(came_ref)


def filter_round(core, spec, kernels, came, which):
    _, conds, _, chunks, _, freqs, count = kernels.shape
    owners = conds * chunks
    mine = pl.BlockSpec(
        (2, conds, None, chunks, None, freqs, count),
        lambda b, own: (0, 0, own[0], 0, which, 0, 0),
    )
    theirs = pl.BlockSpec(
        (2, conds, chunks, None, freqs, count), lambda b, own: (0, 0, 0, which, 0, 0)
    )
    return pl.pallas_call(
        filter_kernel,
        grid_spec=pltpu.PrefetchScalarGridSpec(
            num_scalar_prefetch=1,
            grid=(2,),
            in_specs=[pl.BlockSpec((2, freqs, count), lambda b, own: (0, 0, 0)), mine, theirs],
            out_specs=pl.BlockSpec((owners, 2, freqs, count), lambda b, own: (b, 0, 0, 0)),
        ),
        out_shape=jax.ShapeDtypeStruct((2 * owners, 2, freqs, count), jnp.bfloat16),
        cost_estimate=pl.CostEstimate(
            flops=32 * owners * freqs * freqs * count,
            bytes_accessed=16 * owners * freqs * count,
            transcendentals=0,
        ),
    )(core, spec, kernels, came)


def item_kernel(first, last, weight_ref, parts_ref, wave_ref, back_ref, *rest):
    if first:
        out_ref, mixed, turn = rest
        sum_ref = None
    else:
        sum_ref, out_ref, mixed, turn = rest
    owners, _, freqs, count = parts_ref.shape
    half = freqs // 2
    quarter = count // 2
    width = back_ref.shape[2]

    @pl.when(pl.program_id(0) == 0)
    def _():
        for parity in range(2):
            base = parity * count
            for owner in range(owners):
                at = base + owner * half
                re = parts_ref[owner, 0, parity * half : (parity + 1) * half, :]
                im = parts_ref[owner, 1, parity * half : (parity + 1) * half, :]
                mixed[at : at + half, :count] = re
                mixed[at : at + half, count:] = -im
                mixed[at + quarter : at + quarter + half, :count] = im
                mixed[at + quarter : at + quarter + half, count:] = re
            cos_part = back_ref[2 * parity]
            sin_part = back_ref[2 * parity + 1]
            turn[parity, :quarter, :width] = cos_part
            turn[parity, :quarter, width:] = sin_part
            turn[parity, quarter:, :width] = -sin_part
            turn[parity, quarter:, width:] = cos_part

    halves = lax.dot_general(
        wave_ref[...], mixed[...], (((1,), (1,)), ((), ())), preferred_element_type=jnp.float32
    ).astype(jnp.bfloat16)
    even = jnp.dot(halves[:, :count], turn[0], preferred_element_type=jnp.float32)
    odd = jnp.dot(halves[:, count:], turn[1], preferred_element_type=jnp.float32)
    near = even + odd
    far = even - odd
    weight = weight_ref[0]
    powers = []
    for index, field in enumerate((near, far)):
        re = field[:, :width]
        im = field[:, width:]
        power = weight * (re * re + im * im)
        if not first:
            power = power + sum_ref[:, index * width : (index + 1) * width]
        powers.append(power)
    if not last:
        for index, power in enumerate(powers):
            out_ref[:, index * width : (index + 1) * width] = power
    else:
        total = jnp.concatenate(powers, axis=1)
        across, tall, rows, wide = out_ref.shape
        for k in range(across):
            for t in range(tall):
                out_ref[k, t] = total[t * rows : (t + 1) * rows, k * wide : (k + 1) * wide].astype(
                    out_ref.dtype
                )


def item_round(weight, parts, wave, back, total, last, blocks):
    pixels = wave.shape[0]
    owners, _, freqs, count = parts.shape
    kern, tile = blocks
    rows = pixels // tile
    tall = max(1, 256 // rows)
    step = tall * rows
    steps = pixels // step
    first = total is None
    in_specs = [
        pl.BlockSpec(memory_space=pltpu.SMEM),
        pl.BlockSpec(parts.shape, lambda b: (0, 0, 0, 0)),
        pl.BlockSpec((step, 2 * count), lambda b: (b, 0)),
        pl.BlockSpec(back.shape, lambda b: (0, 0, 0)),
    ]
    args = [weight, parts, wave, back]
    if not first:
        in_specs.append(pl.BlockSpec((step, pixels), lambda b: (b, 0)))
        args.append(total)
    if last:
        out_shape = jax.ShapeDtypeStruct((kern, tile, rows, pixels // kern), jnp.bfloat16)
        out_spec = pl.BlockSpec((kern, tall, rows, pixels // kern), lambda b: (0, b, 0, 0))
    else:
        out_shape = jax.ShapeDtypeStruct((pixels, pixels), jnp.float32)
        out_spec = pl.BlockSpec((step, pixels), lambda b: (b, 0))
    return pl.pallas_call(
        functools.partial(item_kernel, first, last),
        grid=(steps,),
        out_shape=out_shape,
        in_specs=in_specs,
        out_specs=out_spec,
        scratch_shapes=[
            pltpu.VMEM((2 * count, 2 * count), jnp.bfloat16),
            pltpu.VMEM((2, count, pixels), jnp.bfloat16),
        ],
        compiler_params=pltpu.CompilerParams(vmem_limit_bytes=48 * 1024 * 1024),
        cost_estimate=pl.CostEstimate(
            flops=2 * pixels * 4 * count * count + 4 * pixels * pixels * count,
            bytes_accessed=4 * pixels * pixels + 4 * owners * freqs * count,
            transcendentals=0,
        ),
    )(*args)


def local_items(sizes, mask, kernels, kernel_weights):
    tile, kern, cond = sizes
    _, rows, pixels = mask.shape
    freqs, count = kernels.shape[3:]
    conds, kerns = kernel_weights.shape
    items = conds * kerns
    each = items // tile
    cos, sin = host_tables(pixels, count)
    wave = lax.optimization_barrier(
        jnp.asarray(np.concatenate([cos, sin], axis=1), jnp.bfloat16)
    )
    back = jnp.asarray(
        np.stack([part[: pixels // 2, parity::2].T for parity in range(2) for part in (cos, sin)]),
        jnp.bfloat16,
    )
    me = lax.axis_index("tile")
    core = lax.axis_index("cond")
    swap = [(source, 1 - source) for source in range(2)]
    part = kerns // 2
    shares = kernels.reshape(2, conds, 2, part // each, each, freqs, count)
    came = lax.dynamic_index_in_dim(shares, 1 - core, 2, keepdims=False)
    came = lax.ppermute(came, "cond", swap)
    other = lax.ppermute(kernel_weights, "cond", swap)
    weights = jnp.where(
        core == 0,
        jnp.concatenate([kernel_weights, other]),
        jnp.concatenate([other, kernel_weights]),
    )
    weights = lax.dynamic_slice(weights, (0, core * part), (2 * conds, part)).reshape(items)
    weights = lax.dynamic_slice(weights, (me * each,), (each,))
    row = jnp.dot(mask[0], wave, preferred_element_type=jnp.float32)
    row = row.reshape(rows, 2, tile, freqs)
    sign = jnp.asarray([1.0, -1.0], jnp.float32).reshape(1, 2, 1, 1)
    row = (row * sign).astype(jnp.bfloat16)
    row = row.transpose(2, 0, 1, 3).reshape(tile, rows, 2 * freqs)
    cols = lax.all_to_all(row, "tile", split_axis=0, concat_axis=0, tiled=True)
    cols = cols.reshape(pixels, 2 * freqs)
    mixed = lax.dot_general(
        cols, wave, (((0,), (0,)), ((), ())), preferred_element_type=jnp.float32
    )
    spec = jnp.stack(
        [
            mixed[:freqs, :count] + mixed[freqs:, count:],
            mixed[freqs:, :count] - mixed[:freqs, count:],
        ]
    )
    arrived = []
    for index in range(each):
        sent = filter_round(core.reshape(1), spec, shares, came, index)
        arrived.append(lax.all_to_all(sent, "tile", split_axis=0, concat_axis=0, tiled=True))
    total = None
    for index in range(each):
        total = item_round(
            weights[index : index + 1],
            arrived[index],
            wave,
            back,
            total,
            index == each - 1,
            (kern, tile),
        )
    wide = pixels // kern
    total = total.reshape(kern * tile, 2, rows // 2, wide)
    own = lax.dynamic_index_in_dim(total, core, 1, keepdims=False)
    sent = lax.dynamic_index_in_dim(total, 1 - core, 1, keepdims=False)
    got = lax.ppermute(sent, "cond", swap)
    total = (own.astype(jnp.float32) + got.astype(jnp.float32)).astype(jnp.bfloat16)
    blocks = lax.all_to_all(total, ("kern", "tile"), split_axis=0, concat_axis=0, tiled=True)
    blocks = blocks.reshape(kern, 2 * conds, tile // (2 * conds), rows // 2, wide)
    intensity = jnp.sum(blocks.astype(jnp.float32), axis=(0, 2))
    both = jnp.stack([jnp.min(intensity, axis=0), jnp.max(intensity, axis=0)])
    other = lax.ppermute(both, "cond", swap)
    upper = jnp.where(core == 0, both, other)
    lower = jnp.where(core == 0, other, both)
    low = jnp.concatenate([upper[0], lower[0]])
    high = jnp.concatenate([upper[1], lower[1]])
    return (low[None], high[None])


def plan(mesh):
    tile, kern, cond = (mesh.shape[name] for name in ("tile", "kern", "cond"))

    def body(mask, kernels, kernel_weights):
        conds, kerns = kernel_weights.shape
        freqs = kernels.shape[3]
        rows, pixels = mask.shape[1:]
        whole_items = cond == 2 and (conds * kerns) % tile == 0 and tile % (2 * conds) == 0
        whole_items = whole_items and (kerns // 2) % max(1, conds * kerns // tile) == 0
        aligned = freqs % 32 == 0 and rows % 32 == 0 and kerns % 2 == 0 and (pixels // kern) % 128 == 0
        if mask.shape[0] == 1 and whole_items and aligned and kernels.shape[4] * 2 == pixels:
            return local_items((tile, kern, cond), mask, kernels, kernel_weights)
        return local(mask, kernels, kernel_weights)

    return body


def solution(mesh):
    placed = (P(None, "tile", None), P(None, "cond", "kern", "tile", None), P("cond", "kern"))
    return jax.shard_map(
        plan(mesh),
        mesh=mesh,
        in_specs=placed,
        out_specs=(P(None, "tile", "kern"), P(None, "tile", "kern")),
        check_vma=False,
    )
```

```python
import functools
import math

import jax
import jax.numpy as jnp
import numpy as np
from jax import lax
from jax.experimental import pallas as pl
from jax.experimental.pallas import tpu as pltpu
from jax.sharding import PartitionSpec as P


def tables(length, count):
    pixel = jnp.arange(length, dtype=jnp.int32)[:, None]
    freq = jnp.arange(count, dtype=jnp.int32)[None, :] - count // 2
    phase = jnp.mod(pixel * freq, length).astype(jnp.float32) * (2.0 * math.pi / length)
    factor = 1.0 / math.sqrt(length)
    return (
        (jnp.cos(phase) * factor).astype(jnp.bfloat16),
        (jnp.sin(phase) * factor).astype(jnp.bfloat16),
    )


def field_power(half_re, half_im, cos_table, sin_table):
    field_re = jnp.einsum("tnjr,pj->tnrp", half_re, cos_table, preferred_element_type=jnp.float32)
    field_re = field_re - jnp.einsum(
        "tnjr,pj->tnrp", half_im, sin_table, preferred_element_type=jnp.float32
    )
    field_im = jnp.einsum("tnjr,pj->tnrp", half_re, sin_table, preferred_element_type=jnp.float32)
    field_im = field_im + jnp.einsum(
        "tnjr,pj->tnrp", half_im, cos_table, preferred_element_type=jnp.float32
    )
    return field_re * field_re + field_im * field_im


def filter_spectrum(spec_re, spec_im, kern_re, kern_im):
    kern_re = kern_re.astype(jnp.float32)
    kern_im = kern_im.astype(jnp.float32)
    filt_re = spec_re[:, None] * kern_re[None] - spec_im[:, None] * kern_im[None]
    filt_im = spec_re[:, None] * kern_im[None] + spec_im[:, None] * kern_re[None]
    return (filt_re.astype(jnp.bfloat16), filt_im.astype(jnp.bfloat16))


def half_transform(filt_re, filt_im, cos_part, sin_part):
    half_re = jnp.einsum("tnji,ri->tnjr", filt_re, cos_part, preferred_element_type=jnp.float32)
    half_re = half_re - jnp.einsum(
        "tnji,ri->tnjr", filt_im, sin_part, preferred_element_type=jnp.float32
    )
    half_im = jnp.einsum("tnji,ri->tnjr", filt_re, sin_part, preferred_element_type=jnp.float32)
    half_im = half_im + jnp.einsum(
        "tnji,ri->tnjr", filt_im, cos_part, preferred_element_type=jnp.float32
    )
    return (half_re.astype(jnp.bfloat16), half_im.astype(jnp.bfloat16))


def column_spectrum(rows_re, rows_im, cos_part, sin_part):
    spec_re = jnp.einsum("tjr,ri->tji", rows_re, cos_part, preferred_element_type=jnp.float32)
    spec_re = spec_re + jnp.einsum(
        "tjr,ri->tji", rows_im, sin_part, preferred_element_type=jnp.float32
    )
    spec_im = jnp.einsum("tjr,ri->tji", rows_im, cos_part, preferred_element_type=jnp.float32)
    spec_im = spec_im - jnp.einsum(
        "tjr,ri->tji", rows_re, sin_part, preferred_element_type=jnp.float32
    )
    return (spec_re, spec_im)


def local(mask, kernels, kernel_weights):
    tiles_here, rows, pixels = mask.shape
    count = kernels.shape[4]
    conds, kerns = kernel_weights.shape
    items = conds * kerns
    cos_table, sin_table = tables(pixels, count)
    row_re = jnp.einsum("trc,cj->tjr", mask, cos_table, preferred_element_type=jnp.float32).astype(
        jnp.bfloat16
    )
    row_im = (
        -jnp.einsum("trc,cj->tjr", mask, sin_table, preferred_element_type=jnp.float32)
    ).astype(jnp.bfloat16)
    cols_re, cols_im = (
        lax.all_to_all(row_re, "tile", split_axis=1, concat_axis=2, tiled=True),
        lax.all_to_all(row_im, "tile", split_axis=1, concat_axis=2, tiled=True),
    )
    spec_re, spec_im = column_spectrum(cols_re, cols_im, cos_table, sin_table)
    freq_here = kernels.shape[3]
    kern_re = kernels[0].reshape(items, freq_here, count)
    kern_im = kernels[1].reshape(items, freq_here, count)
    filt_re, filt_im = filter_spectrum(spec_re, spec_im, kern_re, kern_im)
    half_re, half_im = half_transform(filt_re, filt_im, cos_table, sin_table)
    power = field_power(
        lax.all_to_all(half_re, "tile", split_axis=3, concat_axis=2, tiled=True),
        lax.all_to_all(half_im, "tile", split_axis=3, concat_axis=2, tiled=True),
        cos_table,
        sin_table,
    )
    power = power.reshape(tiles_here, conds, kerns, rows, pixels)
    weighted = jnp.einsum("tckrp,ck->tcrp", power, kernel_weights, precision=lax.Precision.HIGHEST)
    intensity = lax.psum_scatter(weighted, "kern", scatter_dimension=3, tiled=True)
    local_low = jnp.min(intensity, axis=1)
    local_high = jnp.max(intensity, axis=1)
    low = lax.pmin(local_low, "cond")
    high = lax.pmax(local_high, "cond")
    return (low, high)


def host_tables(length, count):
    pixel = np.arange(length, dtype=np.int64)[:, None]
    freq = np.arange(count, dtype=np.int64)[None, :] - count // 2
    phase = np.mod(pixel * freq, length).astype(np.float64) * (2.0 * math.pi / length)
    factor = 1.0 / math.sqrt(length)
    return np.cos(phase) * factor, np.sin(phase) * factor


def filter_kernel(core_ref, spec_ref, kept_ref, came_ref, out_ref):
    freqs, count = spec_ref.shape[1:]
    half = freqs // 2
    row = lax.broadcasted_iota(jnp.int32, (freqs, freqs), 0)
    col = lax.broadcasted_iota(jnp.int32, (freqs, freqs), 1)
    source = jnp.where(row < half, 2 * row, 2 * (row - half) + 1)
    order = (col == source).astype(jnp.bfloat16)
    spec_re = spec_ref[0]
    spec_im = spec_ref[1]

    def apply(kern_ref):
        chunks = kern_ref.shape[2]
        for part in range(kern_ref.shape[1] * chunks):
            kern_re = kern_ref[0, part // chunks, part % chunks].astype(jnp.float32)
            kern_im = kern_ref[1, part // chunks, part % chunks].astype(jnp.float32)
            filt_re = (spec_re * kern_re - spec_im * kern_im).astype(jnp.bfloat16)
            filt_im = (spec_re * kern_im + spec_im * kern_re).astype(jnp.bfloat16)
            out_ref[part, 0] = jnp.dot(order, filt_re, preferred_element_type=jnp.float32).astype(
                jnp.bfloat16
            )
            out_ref[part, 1] = jnp.dot(order, filt_im, preferred_element_type=jnp.float32).astype(
                jnp.bfloat16
            )

    mine = pl.program_id(0) == core_ref[0]

    @pl.when(mine)
    def _():
        apply(kept_ref)

    @pl.when(jnp.logical_not(mine))
    def _():
        apply(came_ref)


def filter_round(core, spec, kernels, came, which):
    _, conds, _, chunks, _, freqs, count = kernels.shape
    owners = conds * chunks
    mine = pl.BlockSpec(
        (2, conds, None, chunks, None, freqs, count),
        lambda b, own: (0, 0, own[0], 0, which, 0, 0),
    )
    return pl.pallas_call(
        filter_kernel,
        grid_spec=pltpu.PrefetchScalarGridSpec(
            num_scalar_prefetch=1,
            grid=(2,),
            in_specs=[pl.BlockSpec((2, freqs, count), lambda b, own: (0, 0, 0)), mine, mine],
            out_specs=pl.BlockSpec((owners, 2, freqs, count), lambda b, own: (b, 0, 0, 0)),
        ),
        out_shape=jax.ShapeDtypeStruct((2 * owners, 2, freqs, count), jnp.bfloat16),
        cost_estimate=pl.CostEstimate(
            flops=32 * owners * freqs * freqs * count,
            bytes_accessed=16 * owners * freqs * count,
            transcendentals=0,
        ),
    )(core, spec, kernels, came)


def item_kernel(first, last, weight_ref, parts_ref, wave_ref, back_ref, *rest):
    if first:
        out_ref, mixed, turn = rest
        sum_ref = None
    else:
        sum_ref, out_ref, mixed, turn = rest
    owners, _, freqs, count = parts_ref.shape
    half = freqs // 2
    quarter = count // 2
    width = back_ref.shape[2]

    @pl.when(pl.program_id(0) == 0)
    def _():
        for parity in range(2):
            base = parity * count
            for owner in range(owners):
                at = base + owner * half
                re = parts_ref[owner, 0, parity * half : (parity + 1) * half, :]
                im = parts_ref[owner, 1, parity * half : (parity + 1) * half, :]
                mixed[at : at + half, :count] = re
                mixed[at : at + half, count:] = -im
                mixed[at + quarter : at + quarter + half, :count] = im
                mixed[at + quarter : at + quarter + half, count:] = re
            cos_part = back_ref[2 * parity]
            sin_part = back_ref[2 * parity + 1]
            turn[parity, :quarter, :width] = cos_part
            turn[parity, :quarter, width:] = sin_part
            turn[parity, quarter:, :width] = -sin_part
            turn[parity, quarter:, width:] = cos_part

    halves = lax.dot_general(
        wave_ref[...], mixed[...], (((1,), (1,)), ((), ())), preferred_element_type=jnp.float32
    ).astype(jnp.bfloat16)
    even = jnp.dot(halves[:, :count], turn[0], preferred_element_type=jnp.float32)
    odd = jnp.dot(halves[:, count:], turn[1], preferred_element_type=jnp.float32)
    near = even + odd
    far = even - odd
    weight = weight_ref[0]
    powers = []
    for index, field in enumerate((near, far)):
        re = field[:, :width]
        im = field[:, width:]
        power = weight * (re * re + im * im)
        if not first:
            power = power + sum_ref[:, index * width : (index + 1) * width]
        powers.append(power)
    if not last:
        for index, power in enumerate(powers):
            out_ref[:, index * width : (index + 1) * width] = power
    else:
        total = jnp.concatenate(powers, axis=1)
        across, tall, rows, wide = out_ref.shape
        for k in range(across):
            for t in range(tall):
                out_ref[k, t] = total[t * rows : (t + 1) * rows, k * wide : (k + 1) * wide].astype(
                    out_ref.dtype
                )


def item_round(weight, parts, wave, back, total, last, blocks):
    pixels = wave.shape[0]
    owners, _, freqs, count = parts.shape
    kern, tile = blocks
    rows = pixels // tile
    tall = max(1, 256 // rows)
    step = tall * rows
    steps = pixels // step
    first = total is None
    in_specs = [
        pl.BlockSpec(memory_space=pltpu.SMEM),
        pl.BlockSpec(parts.shape, lambda b: (0, 0, 0, 0)),
        pl.BlockSpec((step, 2 * count), lambda b: (b, 0)),
        pl.BlockSpec(back.shape, lambda b: (0, 0, 0)),
    ]
    args = [weight, parts, wave, back]
    if not first:
        in_specs.append(pl.BlockSpec((step, pixels), lambda b: (b, 0)))
        args.append(total)
    if last:
        out_shape = jax.ShapeDtypeStruct((kern, tile, rows, pixels // kern), jnp.bfloat16)
        out_spec = pl.BlockSpec((kern, tall, rows, pixels // kern), lambda b: (0, b, 0, 0))
    else:
        out_shape = jax.ShapeDtypeStruct((pixels, pixels), jnp.float32)
        out_spec = pl.BlockSpec((step, pixels), lambda b: (b, 0))
    return pl.pallas_call(
        functools.partial(item_kernel, first, last),
        grid=(steps,),
        out_shape=out_shape,
        in_specs=in_specs,
        out_specs=out_spec,
        scratch_shapes=[
            pltpu.VMEM((2 * count, 2 * count), jnp.bfloat16),
            pltpu.VMEM((2, count, pixels), jnp.bfloat16),
        ],
        compiler_params=pltpu.CompilerParams(vmem_limit_bytes=48 * 1024 * 1024),
        cost_estimate=pl.CostEstimate(
            flops=2 * pixels * 4 * count * count + 4 * pixels * pixels * count,
            bytes_accessed=4 * pixels * pixels + 4 * owners * freqs * count,
            transcendentals=0,
        ),
    )(*args)


def local_items(sizes, mask, kernels, kernel_weights):
    tile, kern, cond = sizes
    _, rows, pixels = mask.shape
    freqs, count = kernels.shape[3:]
    conds, kerns = kernel_weights.shape
    items = conds * kerns
    each = items // tile
    cos, sin = host_tables(pixels, count)
    wave = lax.optimization_barrier(
        jnp.asarray(np.concatenate([cos, sin], axis=1), jnp.bfloat16)
    )
    back = jnp.asarray(
        np.stack([part[: pixels // 2, parity::2].T for parity in range(2) for part in (cos, sin)]),
        jnp.bfloat16,
    )
    me = lax.axis_index("tile")
    core = lax.axis_index("cond")
    swap = [(source, 1 - source) for source in range(2)]
    part = kerns // 2
    shares = kernels.reshape(2, conds, 2, part // each, each, freqs, count)
    came = lax.ppermute(kernels, "cond", swap).reshape(shares.shape)
    other = lax.ppermute(kernel_weights, "cond", swap)
    weights = jnp.where(
        core == 0,
        jnp.concatenate([kernel_weights, other]),
        jnp.concatenate([other, kernel_weights]),
    )
    weights = lax.dynamic_slice(weights, (0, core * part), (2 * conds, part)).reshape(items)
    weights = lax.dynamic_slice(weights, (me * each,), (each,))
    row = lax.optimization_barrier(jnp.dot(mask[0], wave, preferred_element_type=jnp.float32))
    row = row.reshape(rows, 2, tile, freqs)
    sign = jnp.asarray([1.0, -1.0], jnp.float32).reshape(1, 2, 1, 1)
    row = (row * sign).astype(jnp.bfloat16)
    row = row.transpose(2, 0, 1, 3).reshape(tile, rows, 2 * freqs)
    cols = lax.all_to_all(row, "tile", split_axis=0, concat_axis=0, tiled=True)
    cols = cols.reshape(pixels, 2 * freqs)
    mixed = lax.dot_general(
        cols, wave, (((0,), (0,)), ((), ())), preferred_element_type=jnp.float32
    )
    spec = jnp.stack(
        [
            mixed[:freqs, :count] + mixed[freqs:, count:],
            mixed[freqs:, :count] - mixed[:freqs, count:],
        ]
    )
    arrived = []
    for index in range(each):
        sent = filter_round(core.reshape(1), spec, shares, came, index)
        arrived.append(lax.all_to_all(sent, "tile", split_axis=0, concat_axis=0, tiled=True))
    total = None
    for index in range(each):
        total = item_round(
            weights[index : index + 1],
            arrived[index],
            wave,
            back,
            total,
            index == each - 1,
            (kern, tile),
        )
    wide = pixels // kern
    total = total.reshape(kern * tile, 2, rows // 2, wide)
    own = lax.dynamic_index_in_dim(total, core, 1, keepdims=False)
    sent = lax.dynamic_index_in_dim(total, 1 - core, 1, keepdims=False)
    got = lax.ppermute(sent, "cond", swap)
    total = (own.astype(jnp.float32) + got.astype(jnp.float32)).astype(jnp.bfloat16)
    blocks = lax.all_to_all(total, ("kern", "tile"), split_axis=0, concat_axis=0, tiled=True)
    blocks = blocks.reshape(kern, 2 * conds, tile // (2 * conds), rows // 2, wide)
    intensity = jnp.sum(blocks.astype(jnp.float32), axis=(0, 2))
    both = jnp.stack([jnp.min(intensity, axis=0), jnp.max(intensity, axis=0)])
    other = lax.ppermute(both, "cond", swap)
    upper = jnp.where(core == 0, both, other)
    lower = jnp.where(core == 0, other, both)
    low = jnp.concatenate([upper[0], lower[0]])
    high = jnp.concatenate([upper[1], lower[1]])
    return (low[None], high[None])


def plan(mesh):
    tile, kern, cond = (mesh.shape[name] for name in ("tile", "kern", "cond"))

    def body(mask, kernels, kernel_weights):
        conds, kerns = kernel_weights.shape
        freqs = kernels.shape[3]
        rows, pixels = mask.shape[1:]
        whole_items = cond == 2 and (conds * kerns) % tile == 0 and tile % (2 * conds) == 0
        whole_items = whole_items and (kerns // 2) % max(1, conds * kerns // tile) == 0
        aligned = freqs % 32 == 0 and rows % 32 == 0 and kerns % 2 == 0 and (pixels // kern) % 128 == 0
        if mask.shape[0] == 1 and whole_items and aligned and kernels.shape[4] * 2 == pixels:
            return local_items((tile, kern, cond), mask, kernels, kernel_weights)
        return local(mask, kernels, kernel_weights)

    return body


def solution(mesh):
    placed = (P(None, "tile", None), P(None, "cond", "kern", "tile", None), P("cond", "kern"))
    return jax.shard_map(
        plan(mesh),
        mesh=mesh,
        in_specs=placed,
        out_specs=(P(None, "tile", "kern"), P(None, "tile", "kern")),
        check_vma=False,
    )
```
